256 devices in a mesh: vert: 256 (over z, x, y, core).
Axes of the slice: x: 4, y: 4, z: 8, core: 2. Of those that a mesh axis runs over, the one named last changes fastest.
Arguments:
- feats: bfloat16 [524288, 128], P('vert'), may hold values from -6 to 6
- w_self: bfloat16 [128, 256], replicated, may hold values from -0.5 to 0.5
- w_neigh: bfloat16 [128, 256], replicated, may hold values from -0.5 to 0.5
- bias: float32 [256], replicated, may hold values from -0.6 to 0.6
- cotangent: bfloat16 [524288, 256], P('vert'), may hold values from -24 to 24
- send_rows: int32 [256, 256, 8], P('vert'), may hold values from 0 to 2047
- hub_ids: int32 [368], replicated, may hold values from 0 to 524287, as said below
- edge_src: int32 [256, 16384], P('vert'), may hold values from 0 to 4463, as said below
- edge_dst: int32 [256, 16384], P('vert'), may hold values from 0 to 2047, never falling along the last dimension, each value on 1 to 64 neighbouring positions
- edge_count: int32 [256], P('vert'), may hold values from 1 to 16384, 1677721 in all
Outputs:
- output: bfloat16 [524288, 256], P('vert')
- grad_feats: bfloat16 [524288, 128], P('vert')
- grad_w_self: float32 [128, 256], replicated
- grad_w_neigh: float32 [128, 256], replicated
- grad_bias: float32 [256], replicated
The draws below stay inside these ranges and needn't reach their ends.
Inputs may be any that keep to these rules, and one draw needn't show every extreme that they name: edge_src[d, e] indexes block d's source table: values below 2048 are own rows, values from 2048 to 4095 are halo slots (owner p = (value - 2048) // 8, slot c = (value - 2048) % 8), higher values are hubs (index value - 2048 - 256*8 into hub_ids). hub_ids is strictly ascending; no device's id range holds more than 8 hubs, some device's range holds exactly 8, and every device's range holds at least one.
All inputs are finite; a program needn't handle non-finite values.
Results may differ from the reference program's by a relative error of at most 0.0055.
Values may be sent and summed in bfloat16 or wider, within the bound.
No kernel may reach another device: no remote copies, remote signals or barrier semaphores. Data moves between devices by JAX's collectives and lax.ppermute only.
A program may use at most 64 MiB of HBM per device.

```python
import math
import jax
import jax.numpy as jnp
import numpy as np
from jax import lax

F_IN = 128
F_OUT = 256
V_DEV = 2048
C_REST = 8
HUB_MOST = 8
DEG_MOST = 64
E_DEV = 16384
VERTICES = 524288
HUBS = 368
N_VERT = 256


def pick_places(place_key):
    return jax.random.permutation(place_key, V_DEV)[:HUB_MOST]


def draw_hub_ids(key, part):
    base_key = jax.random.fold_in(key, 23)
    order_key, place_key = jax.random.split(base_key)
    owners = jnp.arange(N_VERT, dtype=jnp.int32)
    ranking = jax.random.permutation(order_key, N_VERT).astype(jnp.int32)
    heavy_count = N_VERT // 16
    hub_counts = jnp.where(ranking < heavy_count, HUB_MOST, 1)
    place_keys = jax.random.split(place_key, N_VERT)
    picked = jax.vmap(pick_places)(place_keys).astype(jnp.int32)
    column = jnp.arange(HUB_MOST, dtype=jnp.int32)
    global_ids = owners[:, None] * V_DEV + picked
    marked = jnp.where(column[None, :] < hub_counts[:, None], global_ids, N_VERT * V_DEV)
    return jnp.sort(marked.reshape(-1))[:HUBS].astype(jnp.int32)


def draw_edge_src(key, part):
    base_key = jax.random.fold_in(key, 41)
    key_list = jax.random.split(base_key, 6)
    grid_shape = (N_VERT, E_DEV)
    category = jax.random.randint(key_list[0], grid_shape, 0, 8)
    local_pick = jax.random.randint(key_list[1], grid_shape, 0, V_DEV)
    halo_pick = V_DEV + jax.random.randint(key_list[2], grid_shape, 0, N_VERT * C_REST)
    draw_one = jax.random.randint(key_list[3], grid_shape, 0, HUBS)
    draw_two = jax.random.randint(key_list[4], grid_shape, 0, HUBS)
    uniform_hub = jax.random.randint(key_list[5], grid_shape, 0, HUBS)
    hub_base = V_DEV + N_VERT * C_REST
    hub_pick = hub_base + jnp.where(category == 6, jnp.minimum(draw_one, draw_two), uniform_hub)
    chosen = jnp.where(category < 3, local_pick, jnp.where(category < 6, halo_pick, hub_pick))
    return chosen.astype(jnp.int32)


def place_ends(array, own_key, low, high):
    spot = [jax.random.randint(jax.random.fold_in(own_key, axis), (), 0, length) for axis, length in enumerate(array.shape)]
    widest = array.shape.index(max(array.shape))
    neighbour = spot[:widest] + [(spot[widest] + 1) % array.shape[widest]] + spot[widest + 1:]
    return array.at[tuple(spot)].set(low).at[tuple(neighbour)].set(high)


def raised(drawn, own_key, source, target, parts, factor):
    def block_of(dim):
        return (jnp.arange(drawn.shape[dim]) // (drawn.shape[dim] // parts)).reshape((-1,) + (1,) * (drawn.ndim - 1 - dim))

    first = jax.random.permutation(own_key, parts)[block_of(target)]
    far = (block_of(target) + parts // 2) % parts
    return jnp.where((block_of(source) == first) | (block_of(source) == far), factor * drawn, drawn)


def level_of(key, extent, pieces, least, largest):
    loudness, own = 1.0, jax.random.fold_in(key, 6)
    for dim, parts in pieces:
        heights = jnp.exp(jax.random.uniform(jax.random.fold_in(own, dim), (parts,), jnp.float32, least / len(pieces), largest / len(pieces)))
        loudness = loudness * jnp.repeat(heights, extent[dim] // parts).reshape([-1 if axis == dim else 1 for axis in range(len(extent))])
    return loudness


def split_up(count, total, limit, lean):
    portions = [(1 << 20) // math.isqrt(standing ** lean) + 1 for standing in range(2, count + 1)]
    rest, given = total - limit - (count - 1), [1] * (count - 1)
    while rest > 0:
        free = [i for i in range(count - 1) if given[i] < limit]
        whole, budget = sum([portions[i] for i in free]), rest
        for i in free:
            extra = min(limit - given[i], max(1, budget * portions[i] // whole), rest)
            given[i] = given[i] + extra
            rest = rest - extra
    return np.array([limit] + given)


def ragged(own_key, count, total, reach, skew):
    if count == 2:
        one = jax.random.randint(own_key, (), max(1, total - reach), min(reach, total - 1) + 1)
        return jnp.stack([one, total - one])
    sizes = jnp.asarray(split_up(count, total, reach, skew), jnp.int32)
    twos = (count - 1) // 2
    source_of, taker = sizes[1:1 + 2 * twos:2], sizes[2:2 + 2 * twos:2]
    slack = jnp.minimum(source_of - 1, reach - taker)
    moved = jax.random.randint(jax.random.fold_in(own_key, 1), (twos,), 0, 1 << 20) % (slack + 1)
    sizes = sizes.at[1:1 + 2 * twos:2].set(source_of - moved).at[2:2 + 2 * twos:2].set(taker + moved)
    return sizes[jax.random.permutation(jax.random.fold_in(own_key, 2), count)]


def centred(rng, shape, width, limit, shards=(), held_as=jnp.bfloat16):
    values = width * jax.random.normal(rng, shape, jnp.float32)
    if shards:
        values = values * level_of(rng, shape, shards, -0.22, 0.18)
    return jnp.clip(values, -limit, limit).astype(held_as)


def noise_with(stream_key, extent, deviation, most, cuts, heavy, kind=jnp.bfloat16):
    values = deviation * jax.random.normal(stream_key, extent, jnp.float32)
    if cuts:
        values = values * level_of(stream_key, extent, cuts, -0.22, 0.18)
    return jnp.clip(raised(values, jax.random.fold_in(stream_key, 3), *heavy), -most, most).astype(kind)


def setup_inputs(seed: int = 0) -> dict:
    seeds = jax.random.split(jax.random.key(seed), 11)
    feats = centred(seeds[0], (VERTICES, F_IN), 1.0, 6.0, ((0, 256),))
    w_self = centred(seeds[1], (F_IN, F_OUT), F_IN ** -0.5, 0.5)
    w_neigh = centred(seeds[2], (F_IN, F_OUT), F_IN ** -0.5, 0.5)
    bias = centred(seeds[3], (F_OUT,), 0.1, 0.6, (), jnp.float32)
    cotangent = noise_with(seeds[4], (VERTICES, F_OUT), 1.0, 24.0, ((0, 256),), (0, 1, 256, 6.0))
    send_rows = place_ends(jax.random.randint(seeds[5], (N_VERT, N_VERT, C_REST), 0, V_DEV), jax.random.fold_in(seeds[5], 1), 0, V_DEV - 1).astype(jnp.int32)
    hub_ids = draw_hub_ids(jax.random.fold_in(seeds[10], 71), 0)
    edge_src = draw_edge_src(jax.random.fold_in(seeds[10], 71), 0)
    edge_dst = jax.vmap(lambda own: jnp.searchsorted(jnp.cumsum(ragged(own, V_DEV, E_DEV, DEG_MOST, 2)), jnp.arange(E_DEV), side="right"))(jax.random.split(seeds[8], N_VERT)).reshape((N_VERT, E_DEV)).astype(jnp.int32)
    edge_count = ragged(seeds[9], N_VERT, N_VERT * E_DEV * 2 // 5, E_DEV, 2).astype(jnp.int32)
    return dict(feats=feats, w_self=w_self, w_neigh=w_neigh, bias=bias, cotangent=cotangent, send_rows=send_rows, hub_ids=hub_ids, edge_src=edge_src, edge_dst=edge_dst, edge_count=edge_count)


def silu_slope(linear):
    logistic = jax.nn.sigmoid(linear)
    return logistic * (1.0 + linear * (1.0 - logistic))


def reference(feats, w_self, w_neigh, bias, cotangent, send_rows, hub_ids, edge_src, edge_dst, edge_count):
    owner_base = jnp.arange(N_VERT, dtype=jnp.int32) * V_DEV
    local_ids = jnp.arange(V_DEV, dtype=jnp.int32)
    edge_ids = jnp.arange(E_DEV, dtype=jnp.int32)
    table_rows = V_DEV + N_VERT * C_REST + HUBS

    def device_step(running, device):
        grad_feats, grad_w_self, grad_w_neigh, grad_bias = running
        block_start = device * V_DEV
        own_feats = lax.dynamic_slice_in_dim(feats, block_start, V_DEV, 0)
        upstream = lax.dynamic_slice_in_dim(cotangent, block_start, V_DEV, 0)
        send_plan = lax.dynamic_index_in_dim(send_rows, device, 1, keepdims=False)
        halo_ids = (owner_base[:, None] + send_plan).reshape(-1).astype(jnp.int32)
        table_ids = jnp.concatenate([(block_start + local_ids).astype(jnp.int32), halo_ids, hub_ids.astype(jnp.int32)])
        source_table = feats[table_ids]
        edge_from = lax.dynamic_index_in_dim(edge_src, device, 0, keepdims=False)
        edge_to = lax.dynamic_index_in_dim(edge_dst, device, 0, keepdims=False)
        real_count = lax.dynamic_index_in_dim(edge_count, device, 0, keepdims=False)
        is_real = edge_ids < real_count
        drop_to = jnp.where(is_real, edge_to, V_DEV)
        degree = jax.ops.segment_sum(is_real.astype(jnp.float32), drop_to, num_segments=V_DEV)
        inverse = 1.0 / jnp.maximum(degree, 1.0)
        summed = jax.ops.segment_sum(source_table[edge_from].astype(jnp.float32), drop_to, num_segments=V_DEV)
        mean_rows = (summed * inverse[:, None]).astype(jnp.bfloat16)
        linear = jnp.dot(own_feats, w_self, preferred_element_type=jnp.float32)
        linear = linear + jnp.dot(mean_rows, w_neigh, preferred_element_type=jnp.float32) + bias
        output = jax.nn.silu(linear).astype(jnp.bfloat16)
        grad_linear = (upstream.astype(jnp.float32) * silu_slope(linear)).astype(jnp.bfloat16)
        grad_w_self = grad_w_self + jnp.dot(own_feats.T, grad_linear, preferred_element_type=jnp.float32)
        grad_w_neigh = grad_w_neigh + jnp.dot(mean_rows.T, grad_linear, preferred_element_type=jnp.float32)
        grad_bias = grad_bias + jnp.sum(grad_linear.astype(jnp.float32), axis=0)
        own_grad = jnp.dot(grad_linear, w_self.T, preferred_element_type=jnp.float32)
        spread = jnp.dot(grad_linear, w_neigh.T, preferred_element_type=jnp.float32) * inverse[:, None]
        drop_from = jnp.where(is_real, edge_from, table_rows)
        back_table = jax.ops.segment_sum(spread[edge_to], drop_from, num_segments=table_rows)
        back_table = back_table.at[:V_DEV].add(own_grad)
        grad_feats = grad_feats.at[table_ids].add(back_table)
        return (grad_feats, grad_w_self, grad_w_neigh, grad_bias), output

    initial = (
        jnp.zeros((V_DEV * N_VERT, F_IN), jnp.float32),
        jnp.zeros((F_IN, F_OUT), jnp.float32),
        jnp.zeros((F_IN, F_OUT), jnp.float32),
        jnp.zeros((F_OUT,), jnp.float32),
    )
    running, blocks = lax.scan(device_step, initial, jnp.arange(N_VERT, dtype=jnp.int32))
    grad_feats, grad_w_self, grad_w_neigh, grad_bias = running
    output = blocks.reshape(V_DEV * N_VERT, F_OUT)
    return (output, grad_feats.astype(jnp.bfloat16), grad_w_self, grad_w_neigh, grad_bias)
```

```python
import jax
import jax.numpy as jnp
from jax import lax
from jax.experimental import pallas as pl
from jax.experimental.pallas import tpu as pltpu
from jax.sharding import PartitionSpec as P

CHUNK = 256
WINDOW = 128
ACCS = 8
ITEMS = 4
BF16 = jnp.bfloat16
F32 = jnp.float32

SMEM = pl.BlockSpec(memory_space=pltpu.SMEM)
VMEM = pl.BlockSpec(memory_space=pltpu.VMEM)


def own_hub(meta_ref, ids_ref, i):
    hub = ids_ref[jnp.minimum(meta_ref[0] + i, ids_ref.shape[0] - 1)]
    return jnp.where(i < meta_ref[1], hub - meta_ref[2], 0)


def pack_kernel(meta_ref, ids_ref, rows_ref, feats_ref, halo_ref, hub_ref, table, picked):
    table[...] = feats_ref[...].astype(F32)

    def chunk(c, carry):
        first = pl.multiple_of(c * CHUNK, CHUNK)
        for e in range(CHUNK):
            picked[pl.ds(e, 1), :] = table[pl.ds(rows_ref[c * CHUNK + e], 1), :]
        halo_ref[pl.ds(first, CHUNK), :] = picked[...].astype(BF16)
        return carry

    lax.fori_loop(0, rows_ref.shape[0] // CHUNK, chunk, 0)
    most = hub_ref.shape[0]
    for i in range(most):
        picked[pl.ds(i, 1), :] = table[pl.ds(own_hub(meta_ref, ids_ref, i), 1), :]
    hub_ref[...] = picked[0:most, :].astype(BF16)


def layer_kernel(
    count_ref, ends_ref, src_ref, place_ref, dst_ref, feats_ref, halo_ref, hubs_ref, cot_ref,
    weights_ref, bias_ref, out_ref, own_ref, send_ref, table, hub_table, picked, sums, spread, wgrad,
    parts, *accs,
):
    local_rows, width = feats_ref.shape
    wide = weights_ref.shape[1]
    halo_rows = halo_ref.shape[0]
    hub_total = place_ref.shape[0]
    hub_base = local_rows + halo_rows
    count = count_ref[0]
    chunks = (count + (CHUNK - 1)) // CHUNK

    table[0:local_rows, :] = feats_ref[...].astype(F32)
    table[local_rows:hub_base, :] = halo_ref[...].astype(F32)
    hub_table[...] = hubs_ref[...].astype(F32)
    for h in range(hub_total):
        table[pl.ds(hub_base + h, 1), :] = hub_table[pl.ds(place_ref[h], 1), :]
    sums[...] = jnp.zeros_like(sums)

    edge_lane = lax.broadcasted_iota(jnp.int32, (1, CHUNK), 1)
    row_id = lax.broadcasted_iota(jnp.int32, (WINDOW, CHUNK), 0)

    def window_of(c):
        low = (ends_ref[2 * c] // 8) * 8
        return low, (ends_ref[2 * c + 1] - low) // WINDOW + 1

    def targets(c):
        row = dst_ref[pl.ds(c, 1), :]
        return jnp.where(edge_lane + c * CHUNK < count, row, -1)

    def forward(c, carry):
        for e in range(CHUNK):
            picked[pl.ds(e, 1), :] = table[pl.ds(src_ref[c * CHUNK + e], 1), :]
        low, blocks = window_of(c)
        rhs = jnp.concatenate([picked[...].astype(BF16), jnp.ones((CHUNK, width), BF16)], axis=1)
        row = targets(c)

        def block(i, inner):
            at = pl.multiple_of(low + i * WINDOW, 8)
            hot = jnp.where(row_id + at == row, 1.0, 0.0).astype(BF16)
            sums[pl.ds(at, WINDOW), :] += jnp.dot(hot, rhs, preferred_element_type=F32)
            return inner

        return lax.fori_loop(0, blocks, block, carry)

    lax.fori_loop(0, chunks, forward, 0)

    wgrad[...] = jnp.zeros_like(wgrad)
    parts[...] = jnp.zeros_like(parts)
    spread[pl.ds(local_rows, WINDOW), :] = jnp.zeros((WINDOW, width), F32)
    weights = weights_ref[...]
    bias = bias_ref[...]

    def dense(b, bias_sum):
        at = pl.multiple_of(b * CHUNK, CHUNK)
        inverse = 1.0 / jnp.maximum(sums[pl.ds(at, CHUNK), width:], 1.0)
        mean = (sums[pl.ds(at, CHUNK), :width] * inverse).astype(BF16)
        both = jnp.concatenate([feats_ref[pl.ds(at, CHUNK), :], mean], axis=1)
        linear = jnp.dot(both, weights, preferred_element_type=F32) + bias
        logistic = jax.nn.sigmoid(linear)
        out_ref[pl.ds(at, CHUNK), :] = (linear * logistic).astype(BF16)
        slope = logistic * (1.0 + linear * (1.0 - logistic))
        grad = (cot_ref[pl.ds(at, CHUNK), :].astype(F32) * slope).astype(BF16)
        wgrad[...] += lax.dot_general(both, grad, (((0,), (0,)), ((), ())), preferred_element_type=F32)
        back = lax.dot_general(grad, weights, (((1,), (1,)), ((), ())), preferred_element_type=F32)
        own_ref[pl.ds(at, CHUNK), :] = back[:, :width]
        spread[pl.ds(at, CHUNK), :] = back[:, width:] * inverse
        return bias_sum + jnp.sum(grad.astype(F32), axis=0, keepdims=True)

    bias_sum = lax.fori_loop(0, local_rows // CHUNK, dense, jnp.zeros((1, wide), F32))

    for acc in accs:
        acc[...] = jnp.zeros_like(acc)

    def backward(c, carry):
        low, blocks = window_of(c)
        row = targets(c)

        def block(i, total):
            at = pl.multiple_of(low + i * WINDOW, 8)
            hot = jnp.where(row_id + at == row, 1.0, 0.0).astype(BF16)
            part = spread[pl.ds(at, WINDOW), :].astype(BF16)
            return total + lax.dot_general(
                hot, part, (((0,), (0,)), ((), ())), preferred_element_type=F32
            )

        picked[...] = lax.fori_loop(0, blocks, block, jnp.zeros((CHUNK, width), F32))
        for e in range(0, CHUNK, ACCS):
            to = [src_ref[c * CHUNK + e + k] for k in range(ACCS)]
            new = [
                accs[k][pl.ds(to[k], 1), :] + picked[pl.ds(e + k, 1), :] for k in range(ACCS)
            ]
            for k in range(ACCS):
                accs[k][pl.ds(to[k], 1), :] = new[k]
        return carry

    lax.fori_loop(0, chunks, backward, 0)

    def total(at, size):
        value = accs[0][pl.ds(at, size), :]
        for acc in accs[1:]:
            value = value + acc[pl.ds(at, size), :]
        return value

    def fold(b, carry):
        at = pl.multiple_of(b * CHUNK, CHUNK)
        own_ref[pl.ds(at, CHUNK), :] += total(at, CHUNK)
        return carry

    lax.fori_loop(0, local_rows // CHUNK, fold, 0)
    peers, depth, _ = send_ref.shape
    slots = halo_rows // peers
    group = CHUNK // slots

    def fold_halo(b, carry):
        at = pl.multiple_of(local_rows + b * CHUNK, CHUNK)
        send_ref[pl.ds(b * group, group), 0:slots, :] = (
            total(at, CHUNK).reshape(group, slots, width).astype(BF16)
        )
        return carry

    lax.fori_loop(0, halo_rows // CHUNK, fold_halo, 0)

    half = 2 * width
    parts[0:half, :] = wgrad[:, :width]
    parts[half : 2 * half, :] = wgrad[:, width:]
    parts[pl.ds(2 * half, 1), :] = bias_sum[:, :width]
    parts[pl.ds(2 * half + 1, 1), :] = bias_sum[:, width:]
    parts[2 * half + 8 : 2 * half + 8 + hub_total, :] = total(hub_base, hub_total)
    for j in range(ITEMS):
        item = parts[j * peers : (j + 1) * peers, :]
        high = item.astype(BF16).astype(F32)
        table[pl.ds(j, peers, stride=2 * ITEMS), :] = high
        table[pl.ds(j + ITEMS, peers, stride=2 * ITEMS), :] = item - high

    def emit(b, carry):
        at = pl.multiple_of(b * CHUNK, CHUNK)
        rows = CHUNK // (2 * ITEMS)
        send_ref[pl.ds(b * rows, rows), slots:, :] = (
            table[pl.ds(at, CHUNK), :].reshape(rows, 2 * ITEMS, width).astype(BF16)
        )
        return carry

    lax.fori_loop(0, peers * 2 * ITEMS // CHUNK, emit, 0)


def finish_kernel(
    meta_ref, ids_ref, rows_ref, own_ref, back_ref, items_ref, grad_ref, self_ref, neigh_ref, bias_ref,
    rows_in, *accs,
):
    local_rows, width = own_ref.shape
    peers, depth, _ = back_ref.shape
    slots = rows_ref.shape[0] // peers
    half = self_ref.shape[0]
    accs[0][...] = own_ref[...]
    for acc in accs[1:]:
        acc[...] = jnp.zeros_like(acc)
    rows_in[...] = back_ref[:, 0:slots, :].astype(F32).reshape(peers * slots, width)

    def chunk(c, carry):
        first = c * CHUNK
        for e in range(0, CHUNK, ACCS):
            to = [rows_ref[first + e + k] for k in range(ACCS)]
            new = [
                accs[k][pl.ds(to[k], 1), :] + rows_in[pl.ds(first + e + k, 1), :]
                for k in range(ACCS)
            ]
            for k in range(ACCS):
                accs[k][pl.ds(to[k], 1), :] = new[k]
        return carry

    lax.fori_loop(0, rows_ref.shape[0] // CHUNK, chunk, 0)
    most = 8
    for i in range(most):
        to = own_hub(meta_ref, ids_ref, i)
        item = 4 * half + 8 + meta_ref[0] + i
        item = jnp.minimum(item, ITEMS * peers - 1)
        row = items_ref[pl.ds((item % peers) * ITEMS + item // peers, 1), :]
        row = jnp.where(i < meta_ref[1], row, 0.0)
        accs[0][pl.ds(to, 1), :] += row

    def fold(b, carry):
        at = pl.multiple_of(b * CHUNK, CHUNK)
        value = accs[0][pl.ds(at, CHUNK), :]
        for acc in accs[1:]:
            value = value + acc[pl.ds(at, CHUNK), :]
        grad_ref[pl.ds(at, CHUNK), :] = value.astype(BF16)
        return carry

    lax.fori_loop(0, local_rows // CHUNK, fold, 0)
    for j in range(2):
        item = items_ref[pl.ds(j, peers, stride=ITEMS), :]
        self_ref[:, j * width : (j + 1) * width] = item[:half]
        neigh_ref[:, j * width : (j + 1) * width] = item[half:]
    for j in range(2):
        bias_ref[:, j * width : (j + 1) * width] = items_ref[pl.ds(j * ITEMS + 2, 1), :]


def body(
    feats, w_self, w_neigh, bias, cotangent, send_rows, hub_ids, edge_src, edge_dst, edge_count
):
    local_rows, width = feats.shape
    wide = w_self.shape[1]
    peers = lax.axis_size("vert")
    own = lax.axis_index("vert")
    slots = send_rows.shape[2]
    hubs = hub_ids.shape[0]
    edges = edge_src.shape[1]
    most = 8
    halo_rows = peers * slots
    table_rows = -(-(local_rows + halo_rows + hubs) // 16) * 16
    owner = hub_ids // local_rows
    lower = jnp.sum(owner[None, :] < owner[:, None], axis=1, dtype=jnp.int32)
    place = owner * most + lax.iota(jnp.int32, hubs) - lower
    first = jnp.sum(owner < own, dtype=jnp.int32)
    held = jnp.sum(owner == own, dtype=jnp.int32)
    slot = lax.iota(jnp.int32, 8)
    meta = jnp.where(slot == 0, first, jnp.where(slot == 1, held, own * local_rows))
    rows = send_rows.reshape(halo_rows)

    halo, own_hubs = pl.pallas_call(
        pack_kernel,
        out_shape=(
            jax.ShapeDtypeStruct((halo_rows, width), BF16),
            jax.ShapeDtypeStruct((most, width), BF16),
        ),
        in_specs=[SMEM, SMEM, SMEM, VMEM],
        out_specs=(VMEM, VMEM),
        scratch_shapes=[pltpu.VMEM((local_rows, width), F32), pltpu.VMEM((CHUNK, width), F32)],
        name="pack",
    )(meta, hub_ids, rows, feats)
    halo = lax.all_to_all(
        halo.reshape(peers, slots, width), "vert", split_axis=0, concat_axis=0, tiled=True
    ).reshape(halo_rows, width)
    hub_rows = lax.all_gather(own_hubs, "vert", axis=0, tiled=True)

    dst = edge_dst.reshape(edges // CHUNK, CHUNK)
    ends = jnp.concatenate([dst[:, :1], dst[:, CHUNK - 1 :]], axis=1).reshape(-1)
    weights = jnp.concatenate([w_self, w_neigh], axis=0)
    output, own_grad, outgoing = pl.pallas_call(
        layer_kernel,
        out_shape=(
            jax.ShapeDtypeStruct((local_rows, wide), BF16),
            jax.ShapeDtypeStruct((local_rows, width), F32),
            jax.ShapeDtypeStruct((peers, slots + 2 * ITEMS, width), BF16),
        ),
        in_specs=[SMEM, SMEM, SMEM, SMEM] + [VMEM] * 7,
        out_specs=(VMEM, VMEM, VMEM),
        scratch_shapes=[
            pltpu.VMEM((table_rows, width), F32),
            pltpu.VMEM((peers * most, width), F32),
            pltpu.VMEM((CHUNK, width), F32),
            pltpu.VMEM((local_rows + 4 * WINDOW, 2 * width), F32),
            pltpu.VMEM((local_rows + WINDOW, width), F32),
            pltpu.VMEM((2 * width, wide), F32),
            pltpu.VMEM((ITEMS * peers, width), F32),
        ]
        + [pltpu.VMEM((table_rows, width), F32)] * ACCS,
        compiler_params=pltpu.CompilerParams(vmem_limit_bytes=56 * 1024 * 1024),
        name="layer",
    )(
        edge_count, ends, edge_src.reshape(edges), place, dst, feats, halo, hub_rows, cotangent,
        weights, bias.reshape(1, wide),
    )
    back = lax.all_to_all(outgoing, "vert", split_axis=0, concat_axis=0, tiled=True)
    summed = jnp.sum(back[:, slots:].astype(F32), axis=0)
    items = lax.all_gather(summed[:ITEMS] + summed[ITEMS:], "vert", axis=0, tiled=True)
    grad_feats, grad_self, grad_neigh, grad_bias = pl.pallas_call(
        finish_kernel,
        out_shape=(
            jax.ShapeDtypeStruct((local_rows, width), BF16),
            jax.ShapeDtypeStruct((width, wide), F32),
            jax.ShapeDtypeStruct((width, wide), F32),
            jax.ShapeDtypeStruct((1, wide), F32),
        ),
        in_specs=[SMEM, SMEM, SMEM] + [VMEM] * 3,
        out_specs=(VMEM,) * 4,
        scratch_shapes=[pltpu.VMEM((halo_rows, width), F32)]
        + [pltpu.VMEM((local_rows, width), F32)] * ACCS,
        name="finish",
    )(meta, hub_ids, rows, own_grad, back, items)
    return (output, grad_feats, grad_self, grad_neigh, grad_bias.reshape(wide))


def solution(mesh):
    in_specs = (
        P("vert", None),
        P(),
        P(),
        P(),
        P("vert", None),
        P("vert", None, None),
        P(),
        P("vert", None),
        P("vert", None),
        P("vert"),
    )
    out_specs = (P("vert", None), P("vert", None), P(), P(), P())
    return jax.shard_map(body, mesh=mesh, in_specs=in_specs, out_specs=out_specs, check_vma=False)
```

```python
import jax
import jax.numpy as jnp
from jax import lax
from jax.experimental import pallas as pl
from jax.experimental.pallas import tpu as pltpu
from jax.sharding import PartitionSpec as P


CHUNK = 256
WINDOW = 128
ACCS = 8
ITEMS = 4
HUB_MOST = 8
BF16 = jnp.bfloat16
F32 = jnp.float32

SMEM = pl.BlockSpec(memory_space=pltpu.SMEM)
VMEM = pl.BlockSpec(memory_space=pltpu.VMEM)


def first_hub(ids_ref, floor):
    total = ids_ref.shape[0]
    low, high = jnp.int32(0), jnp.int32(total)
    for _ in range(total.bit_length()):
        middle = jnp.minimum((low + high) // 2, total - 1)
        below = jnp.logical_and(low < high, ids_ref[middle] < floor)
        above = jnp.logical_and(low < high, jnp.logical_not(below))
        low = jnp.where(below, middle + 1, low)
        high = jnp.where(above, middle, high)
    return low


def own_hub(ids_ref, first, floor, local_rows, i):
    at = jnp.minimum(first + i, ids_ref.shape[0] - 1)
    local = ids_ref[at] - floor
    held = jnp.logical_and(first + i < ids_ref.shape[0], local < local_rows)
    return held, jnp.where(held, local, 0)


def pack_kernel(own_ref, ids_ref, rows_ref, feats_ref, send_ref, table, picked):
    local_rows, width = feats_ref.shape
    peers, depth, _ = send_ref.shape
    slots = rows_ref.shape[0] // peers
    group = CHUNK // slots
    most = depth - slots
    table[...] = feats_ref[...].astype(F32)
    floor = own_ref[0] * local_rows
    first = first_hub(ids_ref, floor)
    for i in range(most):
        _, local = own_hub(ids_ref, first, floor, local_rows, i)
        picked[pl.ds(i, 1), :] = table[pl.ds(local, 1), :]
    hubs = jnp.broadcast_to(picked[0:most, :][None], (group, most, width))

    def chunk(c, carry):
        for e in range(CHUNK):
            picked[pl.ds(e, 1), :] = table[pl.ds(rows_ref[c * CHUNK + e], 1), :]
        halo = picked[...].reshape(group, slots, width)
        both = jnp.concatenate([halo, hubs], axis=1)
        send_ref[pl.ds(c * group, group), :, :] = both.astype(BF16)
        return carry

    lax.fori_loop(0, rows_ref.shape[0] // CHUNK, chunk, 0)


def layer_kernel(
    count_ref, starts_ref, src_ref, ids_ref, dst_ref, feats_ref, come_ref, cot_ref, self_ref,
    neigh_ref, bias_ref, out_ref, own_ref, send_ref, table, come, picked_a, picked_b, sums, spread,
    weights_ref, wgrad, parts, *accs,
):
    local_rows, width = feats_ref.shape
    wide = self_ref.shape[1]
    peers, depth, _ = come_ref.shape
    slots = depth - HUB_MOST
    halo_rows = peers * slots
    hub_total = ids_ref.shape[0]
    hub_base = local_rows + halo_rows
    last_chunk = dst_ref.shape[1] // CHUNK - 1
    count = count_ref[0]
    pairs = (count + (2 * CHUNK - 1)) // (2 * CHUNK)

    table[0:local_rows, :] = feats_ref[...].astype(F32)
    come[...] = come_ref[...].astype(F32).reshape(peers * depth, width)
    table[local_rows:hub_base, :] = (
        come[...].reshape(peers, depth, width)[:, 0:slots, :].reshape(halo_rows, width)
    )
    before, offset = jnp.int32(-1), jnp.int32(0)
    for h in range(hub_total):
        owner = ids_ref[h] // local_rows
        offset = jnp.where(owner == before, offset + 1, 0)
        before = owner
        table[pl.ds(hub_base + h, 1), :] = come[pl.ds(owner * depth + slots + offset, 1), :]
    sums[...] = jnp.zeros_like(sums)

    edge_lane = lax.broadcasted_iota(jnp.int32, (1, CHUNK), 1)
    row_id = lax.broadcasted_iota(jnp.int32, (WINDOW, CHUNK), 0)

    def window_of(c):
        low = (starts_ref[0, c] // 16) * 16
        until = starts_ref[0, jnp.minimum(c + 1, last_chunk)]
        until = jnp.where(c < last_chunk, until, local_rows - 1)
        return low, (until - low) // WINDOW + 1

    def targets(c):
        row = dst_ref[:, pl.ds(pl.multiple_of(c * CHUNK, CHUNK), CHUNK)]
        return jnp.where(edge_lane + c * CHUNK < count, row, -1)

    def one_hot(row, at):
        return jnp.where(row_id + at == row, 1.0, 0.0).astype(BF16)

    def gather(c, into):
        for e in range(CHUNK):
            into[pl.ds(e, 1), :] = table[pl.ds(src_ref[c * CHUNK + e], 1), :]

    def add_up(c, held):
        low, blocks = window_of(c)
        row = targets(c)
        rhs = jnp.concatenate([held[...].astype(BF16), jnp.ones((CHUNK, width), BF16)], axis=1)

        def block(i):
            at = pl.multiple_of(low + i * WINDOW, 16)
            sums[pl.ds(at, WINDOW), :] += jnp.dot(one_hot(row, at), rhs, preferred_element_type=F32)

        block(0)

        def more():
            def step(i, inner):
                block(i)
                return inner

            lax.fori_loop(1, blocks, step, 0)

        return more

    def forward(p, carry):
        for half, held, ahead in ((0, picked_a, picked_b), (1, picked_b, picked_a)):
            c = 2 * p + half
            gather(jnp.minimum(c + 1, last_chunk), ahead)
            add_up(c, held)()
        return carry

    gather(0, picked_a)
    lax.fori_loop(0, pairs, forward, 0)

    wgrad[...] = jnp.zeros_like(wgrad)
    parts[...] = jnp.zeros_like(parts)
    spread[pl.ds(local_rows, WINDOW), :] = jnp.zeros((WINDOW, width), BF16)
    weights_ref[0:width, :] = self_ref[...]
    weights_ref[width:, :] = neigh_ref[...]
    bias = bias_ref[...]

    def dense(b, bias_sum):
        at = pl.multiple_of(b * CHUNK, CHUNK)
        weights = weights_ref[...]
        inverse = 1.0 / jnp.maximum(sums[pl.ds(at, CHUNK), width:], 1.0)
        mean = (sums[pl.ds(at, CHUNK), :width] * inverse).astype(BF16)
        both = jnp.concatenate([feats_ref[pl.ds(at, CHUNK), :], mean], axis=1)
        linear = jnp.dot(both, weights, preferred_element_type=F32) + bias
        logistic = jax.nn.sigmoid(linear)
        out_ref[pl.ds(at, CHUNK), :] = (linear * logistic).astype(BF16)
        slope = logistic * (1.0 + linear * (1.0 - logistic))
        grad = (cot_ref[pl.ds(at, CHUNK), :].astype(F32) * slope).astype(BF16)
        wgrad[...] += lax.dot_general(both, grad, (((0,), (0,)), ((), ())), preferred_element_type=F32)
        back = lax.dot_general(grad, weights, (((1,), (1,)), ((), ())), preferred_element_type=F32)
        own_ref[pl.ds(at, CHUNK), :] = back[:, :width]
        spread[pl.ds(at, CHUNK), :] = (back[:, width:] * inverse).astype(BF16)
        return bias_sum + jnp.sum(grad.astype(F32), axis=0, keepdims=True)

    bias_sum = lax.fori_loop(0, local_rows // CHUNK, dense, jnp.zeros((1, wide), F32))

    for acc in accs:
        acc[...] = jnp.zeros_like(acc)

    def expand(c, into):
        low, blocks = window_of(c)
        row = targets(c)

        def block(i):
            at = pl.multiple_of(low + i * WINDOW, 16)
            return lax.dot_general(
                one_hot(row, at), spread[pl.ds(at, WINDOW), :], (((0,), (0,)), ((), ())),
                preferred_element_type=F32,
            )

        into[...] = block(0)

        def more():
            def step(i, inner):
                into[...] += block(i)
                return inner

            lax.fori_loop(1, blocks, step, 0)

        return more

    def scatter(c, held):
        for e in range(0, CHUNK, ACCS):
            to = [src_ref[c * CHUNK + e + k] for k in range(ACCS)]
            new = [accs[k][pl.ds(to[k], 1), :] + held[pl.ds(e + k, 1), :] for k in range(ACCS)]
            for k in range(ACCS):
                accs[k][pl.ds(to[k], 1), :] = new[k]

    def backward(p, carry):
        for half, held, ahead in ((0, picked_a, picked_b), (1, picked_b, picked_a)):
            c = 2 * p + half
            scatter(c, held)
            expand(jnp.minimum(c + 1, last_chunk), ahead)()
        return carry

    expand(0, picked_a)()
    lax.fori_loop(0, pairs, backward, 0)

    def total(at, size):
        value = accs[0][pl.ds(at, size), :]
        for acc in accs[1:]:
            value = value + acc[pl.ds(at, size), :]
        return value

    def fold(b, carry):
        at = pl.multiple_of(b * CHUNK, CHUNK)
        own_ref[pl.ds(at, CHUNK), :] += total(at, CHUNK)
        return carry

    lax.fori_loop(0, local_rows // CHUNK, fold, 0)
    group = CHUNK // slots

    wide_rows = 2 * width
    parts[0:wide_rows, :] = wgrad[:, :width]
    parts[wide_rows : 2 * wide_rows, :] = wgrad[:, width:]
    parts[pl.ds(2 * wide_rows, 1), :] = bias_sum[:, :width]
    parts[pl.ds(2 * wide_rows + 1, 1), :] = bias_sum[:, width:]
    parts[2 * wide_rows + 8 : 2 * wide_rows + 8 + hub_total, :] = total(hub_base, hub_total)
    for j in range(ITEMS):
        item = parts[j * peers : (j + 1) * peers, :]
        high = item.astype(BF16).astype(F32)
        table[pl.ds(j, peers, stride=2 * ITEMS), :] = high
        table[pl.ds(j + ITEMS, peers, stride=2 * ITEMS), :] = item - high

    def emit(b, carry):
        at = pl.multiple_of(b * CHUNK, CHUNK)
        halo = total(pl.multiple_of(local_rows + at, CHUNK), CHUNK).reshape(group, slots, width)
        items = table[pl.ds(at, CHUNK), :].reshape(group, 2 * ITEMS, width)
        send_ref[pl.ds(b * group, group), :, :] = jnp.concatenate([halo, items], axis=1).astype(BF16)
        return carry

    lax.fori_loop(0, halo_rows // CHUNK, emit, 0)


def finish_kernel(
    floor_ref, shifted_ref, ids_ref, rows_ref, own_ref, back_ref, items_ref, grad_ref, self_ref, neigh_ref,
    bias_ref, rows_in, *accs,
):
    local_rows, width = own_ref.shape
    peers, _, _ = back_ref.shape
    slots = rows_ref.shape[0] // peers
    half = self_ref.shape[0]
    accs[0][...] = own_ref[...]
    for acc in accs[1:]:
        acc[...] = jnp.zeros_like(acc)
    rows_in[...] = back_ref[:, 0:slots, :].astype(F32).reshape(peers * slots, width)

    def chunk(c, carry):
        at = c * CHUNK
        for e in range(0, CHUNK, ACCS):
            to = [rows_ref[at + e + k] for k in range(ACCS)]
            new = [
                accs[k][pl.ds(to[k], 1), :] + rows_in[pl.ds(at + e + k, 1), :]
                for k in range(ACCS)
            ]
            for k in range(ACCS):
                accs[k][pl.ds(to[k], 1), :] = new[k]
        return carry

    lax.fori_loop(0, rows_ref.shape[0] // CHUNK, chunk, 0)
    floor = floor_ref[0]
    first = first_hub(shifted_ref, 0)
    for i in range(HUB_MOST):
        held, to = own_hub(ids_ref, first, floor, local_rows, i)
        item = jnp.where(held, 4 * half + 8 + first + i, 0)
        row = items_ref[pl.ds((item % peers) * ITEMS + item // peers, 1), :]
        row = jnp.where(held, row, 0.0)
        accs[0][pl.ds(to, 1), :] += row

    def fold(b, carry):
        at = pl.multiple_of(b * CHUNK, CHUNK)
        value = accs[0][pl.ds(at, CHUNK), :]
        for acc in accs[1:]:
            value = value + acc[pl.ds(at, CHUNK), :]
        grad_ref[pl.ds(at, CHUNK), :] = value.astype(BF16)
        return carry

    lax.fori_loop(0, local_rows // CHUNK, fold, 0)
    for j in range(2):
        item = items_ref[pl.ds(j, peers, stride=ITEMS), :]
        self_ref[:, j * width : (j + 1) * width] = item[:half]
        neigh_ref[:, j * width : (j + 1) * width] = item[half:]
    for j in range(2):
        bias_ref[:, j * width : (j + 1) * width] = items_ref[pl.ds(j * ITEMS + 2, 1), :]


def exchange(array):
    return lax.all_to_all(array, "vert", split_axis=0, concat_axis=0, tiled=True)


def body(
    feats, w_self, w_neigh, bias, cotangent, send_rows, hub_ids, edge_src, edge_dst, edge_count
):
    local_rows, width = feats.shape
    wide = w_self.shape[1]
    peers = lax.axis_size("vert")
    slots = send_rows.shape[2]
    hubs = hub_ids.shape[0]
    edges = edge_src.shape[1]
    halo_rows = peers * slots
    table_rows = -(-(local_rows + halo_rows + hubs) // 16) * 16
    own = lax.axis_index("vert").astype(jnp.int32).reshape(1)
    rows = send_rows.reshape(halo_rows)

    sent = pl.pallas_call(
        pack_kernel,
        out_shape=jax.ShapeDtypeStruct((peers, slots + HUB_MOST, width), BF16),
        in_specs=[SMEM, SMEM, SMEM, VMEM],
        out_specs=VMEM,
        scratch_shapes=[pltpu.VMEM((local_rows, width), F32), pltpu.VMEM((CHUNK, width), F32)],
        name="pack",
    )(own, hub_ids, rows, feats)
    come = exchange(sent)

    starts = edge_dst[:, ::CHUNK]
    output, own_grad, outgoing = pl.pallas_call(
        layer_kernel,
        out_shape=(
            jax.ShapeDtypeStruct((local_rows, wide), BF16),
            jax.ShapeDtypeStruct((local_rows, width), F32),
            jax.ShapeDtypeStruct((peers, slots + 2 * ITEMS, width), BF16),
        ),
        in_specs=[SMEM, SMEM, SMEM, SMEM] + [VMEM] * 7,
        out_specs=(VMEM, VMEM, VMEM),
        scratch_shapes=[
            pltpu.VMEM((table_rows, width), F32),
            pltpu.VMEM((peers * (slots + HUB_MOST), width), F32),
            pltpu.VMEM((CHUNK, width), F32),
            pltpu.VMEM((CHUNK, width), F32),
            pltpu.VMEM((local_rows + 4 * WINDOW, 2 * width), F32),
            pltpu.VMEM((local_rows + WINDOW, width), BF16),
            pltpu.VMEM((2 * width, wide), BF16),
            pltpu.VMEM((2 * width, wide), F32),
            pltpu.VMEM((ITEMS * peers, width), F32),
        ]
        + [pltpu.VMEM((table_rows, width), F32)] * ACCS,
        compiler_params=pltpu.CompilerParams(vmem_limit_bytes=56 * 1024 * 1024),
        name="layer",
    )(
        edge_count, starts, edge_src.reshape(edges), hub_ids, edge_dst, feats, come, cotangent,
        w_self, w_neigh, bias.reshape(1, wide),
    )
    back = exchange(outgoing)
    hubs_a = hub_ids - own * local_rows
    floors = lax.iota(jnp.int32, 8) + own * local_rows
    summed = jnp.sum(back[:, slots:].astype(F32), axis=0)
    items = (summed[:ITEMS] + summed[ITEMS:])[None]
    items = exchange(jnp.broadcast_to(items, (peers, ITEMS, width)))
    grad_feats, grad_self, grad_neigh, grad_bias = pl.pallas_call(
        finish_kernel,
        out_shape=(
            jax.ShapeDtypeStruct((local_rows, width), BF16),
            jax.ShapeDtypeStruct((width, wide), F32),
            jax.ShapeDtypeStruct((width, wide), F32),
            jax.ShapeDtypeStruct((1, wide), F32),
        ),
        in_specs=[SMEM, SMEM, SMEM, SMEM] + [VMEM] * 3,
        out_specs=(VMEM,) * 4,
        scratch_shapes=[pltpu.VMEM((halo_rows, width), F32)]
        + [pltpu.VMEM((local_rows, width), F32)] * ACCS,
        name="finish",
    )(floors, hubs_a, hub_ids, rows, own_grad, back, items.reshape(peers * ITEMS, width))
    return (output, grad_feats, grad_self, grad_neigh, grad_bias.reshape(wide))


def solution(mesh):
    in_specs = (
        P("vert", None),
        P(),
        P(),
        P(),
        P("vert", None),
        P("vert", None, None),
        P(),
        P("vert", None),
        P("vert", None),
        P("vert"),
    )
    out_specs = (P("vert", None), P("vert", None), P(), P(), P())
    return jax.shard_map(body, mesh=mesh, in_specs=in_specs, out_specs=out_specs, check_vma=False)
```

```python
import jax
import jax.numpy as jnp
from jax import lax
from jax.experimental import pallas as pl
from jax.experimental.pallas import tpu as pltpu
from jax.sharding import PartitionSpec as P


CHUNK = 256
WINDOW = 128
ACCS = 8
HUB_MOST = 8
BF16 = jnp.bfloat16
F32 = jnp.float32

SMEM = pl.BlockSpec(memory_space=pltpu.SMEM)
VMEM = pl.BlockSpec(memory_space=pltpu.VMEM)


def first_hub(ids_ref, floor):
    total = ids_ref.shape[0]
    low, high = jnp.int32(0), jnp.int32(total)
    for _ in range(total.bit_length()):
        middle = jnp.minimum((low + high) // 2, total - 1)
        below = jnp.logical_and(low < high, ids_ref[middle] < floor)
        above = jnp.logical_and(low < high, jnp.logical_not(below))
        low = jnp.where(below, middle + 1, low)
        high = jnp.where(above, middle, high)
    return low


def own_hub(ids_ref, first, floor, local_rows, i):
    at = jnp.minimum(first + i, ids_ref.shape[0] - 1)
    local = ids_ref[at] - floor
    held = jnp.logical_and(first + i < ids_ref.shape[0], local < local_rows)
    return held, jnp.where(held, local, 0)


def pack_kernel(own_ref, ids_ref, rows_ref, feats_ref, send_ref, table, picked):
    local_rows, width = feats_ref.shape
    peers, depth, _ = send_ref.shape
    slots = rows_ref.shape[0] // peers
    group = CHUNK // slots
    most = depth - slots
    table[...] = feats_ref[...].astype(F32)
    floor = own_ref[0] * local_rows
    first = first_hub(ids_ref, floor)
    for i in range(most):
        _, local = own_hub(ids_ref, first, floor, local_rows, i)
        picked[pl.ds(i, 1), :] = table[pl.ds(local, 1), :]
    hubs = jnp.broadcast_to(picked[0:most, :][None], (group, most, width))

    def chunk(c, carry):
        for e in range(CHUNK):
            picked[pl.ds(e, 1), :] = table[pl.ds(rows_ref[c * CHUNK + e], 1), :]
        halo = picked[...].reshape(group, slots, width)
        both = jnp.concatenate([halo, hubs], axis=1)
        send_ref[pl.ds(c * group, group), :, :] = both.astype(BF16)
        return carry

    lax.fori_loop(0, rows_ref.shape[0] // CHUNK, chunk, 0)


def window_of(starts_ref, c, last_chunk, last_row):
    low = (starts_ref[0, c] // 16) * 16
    until = starts_ref[0, jnp.minimum(c + 1, last_chunk)]
    until = jnp.where(c < last_chunk, until, last_row)
    return low, (until - low) // WINDOW + 1


def targets_of(dst_ref, c, count):
    lane = lax.broadcasted_iota(jnp.int32, (1, CHUNK), 1)
    row = dst_ref[:, pl.ds(pl.multiple_of(c * CHUNK, CHUNK), CHUNK)]
    return jnp.where(lane + c * CHUNK < count, row, -1)


def one_hot(row, at):
    row_id = lax.broadcasted_iota(jnp.int32, (WINDOW, CHUNK), 0)
    return jnp.where(row_id + at == row, 1.0, 0.0).astype(BF16)


def forward_kernel(
    count_ref, starts_ref, src_ref, ids_ref, dst_ref, from_ref, feats_ref, come_ref, cot_ref, self_ref,
    neigh_ref, bias_ref, out_ref, own_ref, spread_ref, send_ref, table, come, picked_a, picked_b, sums,
    hub_counts, hub_grads, weights_ref, wgrad,
):
    local_rows, width = feats_ref.shape
    wide = self_ref.shape[1]
    peers, depth, _ = come_ref.shape
    slots = depth - HUB_MOST
    halo_rows = peers * slots
    hub_total = ids_ref.shape[0]
    hub_wide = hub_counts.shape[1]
    hub_base = local_rows + halo_rows
    last_chunk = dst_ref.shape[1] // CHUNK - 1
    count = count_ref[0]
    pairs = (count + (2 * CHUNK - 1)) // (2 * CHUNK)

    table[0:local_rows, :] = feats_ref[...].astype(F32)
    come[...] = come_ref[...].astype(F32).reshape(peers * depth, width)
    table[local_rows:hub_base, :] = (
        come[...].reshape(peers, depth, width)[:, 0:slots, :].reshape(halo_rows, width)
    )
    before, offset = jnp.int32(-1), jnp.int32(0)
    for h in range(hub_total):
        owner = ids_ref[h] // local_rows
        offset = jnp.where(owner == before, offset + 1, 0)
        before = owner
        table[pl.ds(hub_base + h, 1), :] = come[pl.ds(owner * depth + slots + offset, 1), :]
    sums[...] = jnp.zeros_like(sums)
    hub_counts[...] = jnp.zeros_like(hub_counts)
    hub_id = lax.broadcasted_iota(jnp.int32, (hub_wide, CHUNK), 0) + hub_base

    def gather(c, into):
        for e in range(CHUNK):
            into[pl.ds(e, 1), :] = table[pl.ds(src_ref[c * CHUNK + e], 1), :]

    def add_up(c, held):
        low, blocks = window_of(starts_ref, c, last_chunk, local_rows - 1)
        row = targets_of(dst_ref, c, count)
        source = from_ref[:, pl.ds(pl.multiple_of(c * CHUNK, CHUNK), CHUNK)]
        hub_hot = jnp.where(hub_id == source, 1.0, 0.0).astype(BF16)
        rhs = jnp.concatenate([held[...].astype(BF16), jnp.ones((CHUNK, width), BF16)], axis=1)

        def block(i):
            at = pl.multiple_of(low + i * WINDOW, 16)
            hot = one_hot(row, at)
            sums[pl.ds(at, WINDOW), :] += jnp.dot(hot, rhs, preferred_element_type=F32)
            hub_counts[pl.ds(at, WINDOW), :] += lax.dot_general(
                hot, hub_hot, (((1,), (1,)), ((), ())), preferred_element_type=F32
            )

        block(0)

        def step(i, inner):
            block(i)
            return inner

        lax.fori_loop(1, blocks, step, 0)

    def forward(p, carry):
        for half, held, ahead in ((0, picked_a, picked_b), (1, picked_b, picked_a)):
            c = 2 * p + half
            gather(jnp.minimum(c + 1, last_chunk), ahead)
            add_up(c, held)
        return carry

    gather(0, picked_a)
    lax.fori_loop(0, pairs, forward, 0)

    wgrad[...] = jnp.zeros_like(wgrad)
    hub_grads[...] = jnp.zeros_like(hub_grads)
    weights_ref[0:width, :] = self_ref[...]
    weights_ref[width:, :] = neigh_ref[...]
    bias = bias_ref[...]

    def dense(b, bias_sum):
        at = pl.multiple_of(b * CHUNK, CHUNK)
        weights = weights_ref[...]
        inverse = 1.0 / jnp.maximum(sums[pl.ds(at, CHUNK), width:], 1.0)
        mean = (sums[pl.ds(at, CHUNK), :width] * inverse).astype(BF16)
        both = jnp.concatenate([feats_ref[pl.ds(at, CHUNK), :], mean], axis=1)
        linear = jnp.dot(both, weights, preferred_element_type=F32) + bias
        logistic = jax.nn.sigmoid(linear)
        out_ref[pl.ds(at, CHUNK), :] = (linear * logistic).astype(BF16)
        slope = logistic * (1.0 + linear * (1.0 - logistic))
        grad = (cot_ref[pl.ds(at, CHUNK), :].astype(F32) * slope).astype(BF16)
        wgrad[...] += lax.dot_general(both, grad, (((0,), (0,)), ((), ())), preferred_element_type=F32)
        back = lax.dot_general(grad, weights, (((1,), (1,)), ((), ())), preferred_element_type=F32)
        own_ref[pl.ds(at, CHUNK), :] = back[:, :width]
        spread = (back[:, width:] * inverse).astype(BF16)
        spread_ref[pl.ds(at, CHUNK), :] = spread
        hub_grads[...] += lax.dot_general(
            hub_counts[pl.ds(at, CHUNK), :].astype(BF16), spread, (((0,), (0,)), ((), ())),
            preferred_element_type=F32,
        )
        return bias_sum + jnp.sum(grad.astype(F32), axis=0, keepdims=True)

    bias_sum = lax.fori_loop(0, local_rows // CHUNK, dense, jnp.zeros((1, wide), F32))

    come[...] = jnp.zeros_like(come)
    before, offset = jnp.int32(-1), jnp.int32(0)
    for h in range(hub_total):
        owner = ids_ref[h] // local_rows
        offset = jnp.where(owner == before, offset + 1, 0)
        before = owner
        come[pl.ds(owner * depth + offset, 1), :] = hub_grads[pl.ds(h, 1), :]
    for j in range(2):
        for k, value in ((0, wgrad[:, j * width : (j + 1) * width]), (4, bias_sum[:, j * width : (j + 1) * width])):
            high = value.astype(BF16).astype(F32)
            at = HUB_MOST + k + j
            come[pl.ds(at, peers, stride=depth), :] = jnp.broadcast_to(high, (peers, width))
            come[pl.ds(at + 2, peers, stride=depth), :] = jnp.broadcast_to(value - high, (peers, width))
    group = CHUNK // depth

    def emit(b, carry):
        at = pl.multiple_of(b * CHUNK, CHUNK)
        send_ref[pl.ds(b * group, group), :, :] = (
            come[pl.ds(at, CHUNK), :].reshape(group, depth, width).astype(BF16)
        )
        return carry

    lax.fori_loop(0, peers * depth // CHUNK, emit, 0)


def backward_kernel(
    count_ref, starts_ref, src_ref, dst_ref, spread_ref, own_ref, sum_ref, send_ref, spread, picked_a,
    picked_b, *accs,
):
    local_rows, width = own_ref.shape
    peers, slots, _ = send_ref.shape
    halo_rows = peers * slots
    last_chunk = dst_ref.shape[1] // CHUNK - 1
    count = count_ref[0]
    pairs = (count + (2 * CHUNK - 1)) // (2 * CHUNK)
    spread[0:local_rows, :] = spread_ref[...]
    spread[pl.ds(local_rows, WINDOW), :] = jnp.zeros((WINDOW, width), BF16)
    for acc in accs:
        acc[...] = jnp.zeros_like(acc)

    def expand(c, into):
        low, blocks = window_of(starts_ref, c, last_chunk, local_rows - 1)
        row = targets_of(dst_ref, c, count)

        def block(i):
            at = pl.multiple_of(low + i * WINDOW, 16)
            return lax.dot_general(
                one_hot(row, at), spread[pl.ds(at, WINDOW), :], (((0,), (0,)), ((), ())),
                preferred_element_type=F32,
            )

        into[...] = block(0)

        def step(i, inner):
            into[...] += block(i)
            return inner

        lax.fori_loop(1, blocks, step, 0)

    def scatter(c, held):
        for e in range(0, CHUNK, ACCS):
            to = [src_ref[c * CHUNK + e + k] for k in range(ACCS)]
            new = [accs[k][pl.ds(to[k], 1), :] + held[pl.ds(e + k, 1), :] for k in range(ACCS)]
            for k in range(ACCS):
                accs[k][pl.ds(to[k], 1), :] = new[k]

    def backward(p, carry):
        for half, held, ahead in ((0, picked_a, picked_b), (1, picked_b, picked_a)):
            c = 2 * p + half
            scatter(c, held)
            expand(jnp.minimum(c + 1, last_chunk), ahead)
        return carry

    expand(0, picked_a)
    lax.fori_loop(0, pairs, backward, 0)

    def total(at, size):
        value = accs[0][pl.ds(at, size), :]
        for acc in accs[1:]:
            value = value + acc[pl.ds(at, size), :]
        return value

    group = CHUNK // slots

    def fold(b, carry):
        at = pl.multiple_of(b * CHUNK, CHUNK)
        sum_ref[pl.ds(at, CHUNK), :] = own_ref[pl.ds(at, CHUNK), :] + total(at, CHUNK)
        return carry

    def emit(b, carry):
        at = pl.multiple_of(local_rows + b * CHUNK, CHUNK)
        send_ref[pl.ds(b * group, group), :, :] = (
            total(at, CHUNK).reshape(group, slots, width).astype(BF16)
        )
        return carry

    lax.fori_loop(0, local_rows // CHUNK, fold, 0)
    lax.fori_loop(0, halo_rows // CHUNK, emit, 0)


def finish_kernel(own_index_ref, ids_ref, rows_ref, own_ref, back_ref, hubs_ref, grad_ref, rows_in, *accs):
    local_rows, width = own_ref.shape
    peers, slots, _ = back_ref.shape
    accs[0][...] = own_ref[...]
    for acc in accs[1:]:
        acc[...] = jnp.zeros_like(acc)
    rows_in[...] = back_ref[...].astype(F32).reshape(peers * slots, width)

    def chunk(c, carry):
        at = c * CHUNK
        for e in range(0, CHUNK, ACCS):
            to = [rows_ref[at + e + k] for k in range(ACCS)]
            new = [
                accs[k][pl.ds(to[k], 1), :] + rows_in[pl.ds(at + e + k, 1), :]
                for k in range(ACCS)
            ]
            for k in range(ACCS):
                accs[k][pl.ds(to[k], 1), :] = new[k]
        return carry

    lax.fori_loop(0, rows_ref.shape[0] // CHUNK, chunk, 0)
    floor = own_index_ref[0] * local_rows
    first = first_hub(ids_ref, floor)
    for i in range(HUB_MOST):
        held, to = own_hub(ids_ref, first, floor, local_rows, i)
        accs[0][pl.ds(to, 1), :] += jnp.where(held, hubs_ref[pl.ds(i, 1), :], 0.0)

    def fold(b, carry):
        at = pl.multiple_of(b * CHUNK, CHUNK)
        value = accs[0][pl.ds(at, CHUNK), :]
        for acc in accs[1:]:
            value = value + acc[pl.ds(at, CHUNK), :]
        grad_ref[pl.ds(at, CHUNK), :] = value.astype(BF16)
        return carry

    lax.fori_loop(0, local_rows // CHUNK, fold, 0)


def exchange(array):
    return lax.all_to_all(array, "vert", split_axis=0, concat_axis=0, tiled=True)


def body(
    feats, w_self, w_neigh, bias, cotangent, send_rows, hub_ids, edge_src, edge_dst, edge_count
):
    local_rows, width = feats.shape
    wide = w_self.shape[1]
    peers = lax.axis_size("vert")
    slots = send_rows.shape[2]
    hubs = hub_ids.shape[0]
    edges = edge_src.shape[1]
    halo_rows = peers * slots
    table_rows = -(-(local_rows + halo_rows + hubs) // 16) * 16
    own = lax.axis_index("vert").astype(jnp.int32).reshape(1)
    rows = send_rows.reshape(halo_rows)

    sent = pl.pallas_call(
        pack_kernel,
        out_shape=jax.ShapeDtypeStruct((peers, slots + HUB_MOST, width), BF16),
        in_specs=[SMEM, SMEM, SMEM, VMEM],
        out_specs=VMEM,
        scratch_shapes=[pltpu.VMEM((local_rows, width), F32), pltpu.VMEM((CHUNK, width), F32)],
        name="pack",
    )(own, hub_ids, rows, feats)
    come = exchange(sent)

    starts = edge_dst[:, ::CHUNK]
    vmem = pltpu.CompilerParams(vmem_limit_bytes=56 * 1024 * 1024)
    source = edge_src.reshape(edges)
    depth = slots + HUB_MOST
    hub_wide = -(-hubs // 128) * 128
    output, own_grad, spread, items = pl.pallas_call(
        forward_kernel,
        out_shape=(
            jax.ShapeDtypeStruct((local_rows, wide), BF16),
            jax.ShapeDtypeStruct((local_rows, width), F32),
            jax.ShapeDtypeStruct((local_rows, width), BF16),
            jax.ShapeDtypeStruct((peers, depth, width), BF16),
        ),
        in_specs=[SMEM, SMEM, SMEM, SMEM] + [VMEM] * 8,
        out_specs=(VMEM,) * 4,
        scratch_shapes=[
            pltpu.VMEM((table_rows, width), F32),
            pltpu.VMEM((peers * depth, width), F32),
            pltpu.VMEM((CHUNK, width), F32),
            pltpu.VMEM((CHUNK, width), F32),
            pltpu.VMEM((local_rows + 4 * WINDOW, 2 * width), F32),
            pltpu.VMEM((local_rows + 4 * WINDOW, hub_wide), F32),
            pltpu.VMEM((hub_wide, width), F32),
            pltpu.VMEM((2 * width, wide), BF16),
            pltpu.VMEM((2 * width, wide), F32),
        ],
        compiler_params=vmem,
        name="forward",
    )(
        edge_count, starts, source, hub_ids, edge_dst, edge_src, feats, come, cotangent,
        w_self, w_neigh, bias.reshape(1, wide),
    )
    items = exchange(items)
    own_grad, outgoing = pl.pallas_call(
        backward_kernel,
        out_shape=(
            jax.ShapeDtypeStruct((local_rows, width), F32),
            jax.ShapeDtypeStruct((peers, slots, width), BF16),
        ),
        in_specs=[SMEM, SMEM, SMEM] + [VMEM] * 3,
        out_specs=(VMEM, VMEM),
        scratch_shapes=[
            pltpu.VMEM((local_rows + WINDOW, width), BF16),
            pltpu.VMEM((CHUNK, width), F32),
            pltpu.VMEM((CHUNK, width), F32),
        ]
        + [pltpu.VMEM((table_rows, width), F32)] * ACCS,
        compiler_params=vmem,
        name="backward",
    )(edge_count, starts, source, edge_dst, spread, own_grad)
    back = exchange(outgoing)
    summed = jnp.sum(items.astype(F32), axis=0)
    at = HUB_MOST
    mine = (summed[at : at + 2] + summed[at + 2 : at + 4])[None]
    grad_bias = (summed[at + 4 : at + 6] + summed[at + 6 : at + 8]).reshape(wide)
    shared = exchange(jnp.broadcast_to(mine, (peers, 2, width)))
    grad_feats = pl.pallas_call(
        finish_kernel,
        out_shape=jax.ShapeDtypeStruct((local_rows, width), BF16),
        in_specs=[SMEM, SMEM, SMEM] + [VMEM] * 3,
        out_specs=VMEM,
        scratch_shapes=[pltpu.VMEM((halo_rows, width), F32)]
        + [pltpu.VMEM((local_rows, width), F32)] * ACCS,
        name="finish",
    )(own, hub_ids, rows, own_grad, back, summed[:HUB_MOST])
    shared = shared.reshape(2 * width, wide)
    return (output, grad_feats, shared[:width], shared[width:], grad_bias)


def solution(mesh):
    in_specs = (
        P("vert", None),
        P(),
        P(),
        P(),
        P("vert", None),
        P("vert", None, None),
        P(),
        P("vert", None),
        P("vert", None),
        P("vert"),
    )
    out_specs = (P("vert", None), P("vert", None), P(), P(), P())
    return jax.shard_map(body, mesh=mesh, in_specs=in_specs, out_specs=out_specs, check_vma=False)
```

```python
import jax
import jax.numpy as jnp
from jax import lax
from jax.experimental import pallas as pl
from jax.experimental.pallas import tpu as pltpu
from jax.sharding import PartitionSpec as P


CHUNK = 256
WINDOW = 128
ACCS = 8
ITEMS = 4
HUB_MOST = 8
BF16 = jnp.bfloat16
F32 = jnp.float32

SMEM = pl.BlockSpec(memory_space=pltpu.SMEM)
VMEM = pl.BlockSpec(memory_space=pltpu.VMEM)


def first_hub(ids_ref, floor):
    total = ids_ref.shape[0]
    low, high = jnp.int32(0), jnp.int32(total)
    for _ in range(total.bit_length()):
        middle = jnp.minimum((low + high) // 2, total - 1)
        below = jnp.logical_and(low < high, ids_ref[middle] < floor)
        above = jnp.logical_and(low < high, jnp.logical_not(below))
        low = jnp.where(below, middle + 1, low)
        high = jnp.where(above, middle, high)
    return low


def own_hub(ids_ref, first, floor, local_rows, i):
    at = jnp.minimum(first + i, ids_ref.shape[0] - 1)
    local = ids_ref[at] - floor
    held = jnp.logical_and(first + i < ids_ref.shape[0], local < local_rows)
    return held, jnp.where(held, local, 0)


def pack_kernel(own_ref, ids_ref, rows_ref, feats_ref, send_ref, table, picked):
    local_rows, width = feats_ref.shape
    peers, depth, _ = send_ref.shape
    slots = rows_ref.shape[0] // peers
    group = CHUNK // slots
    most = depth - slots
    table[...] = feats_ref[...].astype(F32)
    floor = own_ref[0] * local_rows
    first = first_hub(ids_ref, floor)
    for i in range(most):
        _, local = own_hub(ids_ref, first, floor, local_rows, i)
        picked[pl.ds(i, 1), :] = table[pl.ds(local, 1), :]
    hubs = jnp.broadcast_to(picked[0:most, :][None], (group, most, width))

    def chunk(c, carry):
        for e in range(CHUNK):
            picked[pl.ds(e, 1), :] = table[pl.ds(rows_ref[c * CHUNK + e], 1), :]
        halo = picked[...].reshape(group, slots, width)
        both = jnp.concatenate([halo, hubs], axis=1)
        send_ref[pl.ds(c * group, group), :, :] = both.astype(BF16)
        return carry

    lax.fori_loop(0, rows_ref.shape[0] // CHUNK, chunk, 0)


def layer_kernel(
    count_ref, starts_ref, src_ref, ids_ref, dst_ref, feats_ref, come_ref, cot_ref, self_ref,
    neigh_ref, bias_ref, out_ref, own_ref, send_ref, table, come, picked_a, picked_b, sums, spread,
    weights_ref, wgrad, parts, *accs,
):
    local_rows, width = feats_ref.shape
    wide = self_ref.shape[1]
    peers, depth, _ = come_ref.shape
    slots = depth - HUB_MOST
    halo_rows = peers * slots
    hub_total = ids_ref.shape[0]
    hub_base = local_rows + halo_rows
    last_chunk = dst_ref.shape[1] // CHUNK - 1
    count = count_ref[0]
    pairs = (count + (2 * CHUNK - 1)) // (2 * CHUNK)

    table[0:local_rows, :] = feats_ref[...].astype(F32)
    come[...] = come_ref[...].astype(F32).reshape(peers * depth, width)
    table[local_rows:hub_base, :] = (
        come[...].reshape(peers, depth, width)[:, 0:slots, :].reshape(halo_rows, width)
    )
    before, offset = jnp.int32(-1), jnp.int32(0)
    for h in range(hub_total):
        owner = ids_ref[h] // local_rows
        offset = jnp.where(owner == before, offset + 1, 0)
        before = owner
        table[pl.ds(hub_base + h, 1), :] = come[pl.ds(owner * depth + slots + offset, 1), :]
    sums[...] = jnp.zeros_like(sums)

    edge_lane = lax.broadcasted_iota(jnp.int32, (1, CHUNK), 1)
    row_id = lax.broadcasted_iota(jnp.int32, (WINDOW, CHUNK), 0)

    def window_of(c):
        low = (starts_ref[0, c] // 16) * 16
        until = starts_ref[0, jnp.minimum(c + 1, last_chunk)]
        until = jnp.where(c < last_chunk, until, local_rows - 1)
        return low, (until - low) // WINDOW + 1

    def targets(c):
        row = dst_ref[:, pl.ds(pl.multiple_of(c * CHUNK, CHUNK), CHUNK)]
        return jnp.where(edge_lane + c * CHUNK < count, row, -1)

    def one_hot(row, at):
        return jnp.where(row_id + at == row, 1.0, 0.0).astype(BF16)

    def gather(c, into):
        for e in range(CHUNK):
            into[pl.ds(e, 1), :] = table[pl.ds(src_ref[c * CHUNK + e], 1), :]

    def add_up(c, held):
        low, blocks = window_of(c)
        row = targets(c)
        rhs = jnp.concatenate([held[...].astype(BF16), jnp.ones((CHUNK, width), BF16)], axis=1)

        def block(i):
            at = pl.multiple_of(low + i * WINDOW, 16)
            sums[pl.ds(at, WINDOW), :] += jnp.dot(one_hot(row, at), rhs, preferred_element_type=F32)

        block(0)

        def more():
            def step(i, inner):
                block(i)
                return inner

            lax.fori_loop(1, blocks, step, 0)

        return more

    def forward(p, carry):
        for half, held, ahead in ((0, picked_a, picked_b), (1, picked_b, picked_a)):
            c = 2 * p + half
            gather(jnp.minimum(c + 1, last_chunk), ahead)
            add_up(c, held)()
        return carry

    gather(0, picked_a)
    lax.fori_loop(0, pairs, forward, 0)

    wgrad[...] = jnp.zeros_like(wgrad)
    parts[...] = jnp.zeros_like(parts)
    spread[pl.ds(local_rows, WINDOW), :] = jnp.zeros((WINDOW, width), BF16)
    weights_ref[0:width, :] = self_ref[...]
    weights_ref[width:, :] = neigh_ref[...]
    bias = bias_ref[...]

    def dense(b, bias_sum):
        at = pl.multiple_of(b * CHUNK, CHUNK)
        weights = weights_ref[...]
        inverse = 1.0 / jnp.maximum(sums[pl.ds(at, CHUNK), width:], 1.0)
        mean = (sums[pl.ds(at, CHUNK), :width] * inverse).astype(BF16)
        both = jnp.concatenate([feats_ref[pl.ds(at, CHUNK), :], mean], axis=1)
        linear = jnp.dot(both, weights, preferred_element_type=F32) + bias
        logistic = jax.nn.sigmoid(linear)
        out_ref[pl.ds(at, CHUNK), :] = (linear * logistic).astype(BF16)
        slope = logistic * (1.0 + linear * (1.0 - logistic))
        grad = (cot_ref[pl.ds(at, CHUNK), :].astype(F32) * slope).astype(BF16)
        wgrad[...] += lax.dot_general(both, grad, (((0,), (0,)), ((), ())), preferred_element_type=F32)
        back = lax.dot_general(grad, weights, (((1,), (1,)), ((), ())), preferred_element_type=F32)
        own_ref[pl.ds(at, CHUNK), :] = back[:, :width]
        spread[pl.ds(at, CHUNK), :] = (back[:, width:] * inverse).astype(BF16)
        return bias_sum + jnp.sum(grad.astype(F32), axis=0, keepdims=True)

    bias_sum = lax.fori_loop(0, local_rows // CHUNK, dense, jnp.zeros((1, wide), F32))

    for acc in accs:
        acc[...] = jnp.zeros_like(acc)

    def expand(c, into):
        low, blocks = window_of(c)
        row = targets(c)

        def block(i):
            at = pl.multiple_of(low + i * WINDOW, 16)
            return lax.dot_general(
                one_hot(row, at), spread[pl.ds(at, WINDOW), :], (((0,), (0,)), ((), ())),
                preferred_element_type=F32,
            )

        into[...] = block(0)

        def more():
            def step(i, inner):
                into[...] += block(i)
                return inner

            lax.fori_loop(1, blocks, step, 0)

        return more

    def scatter(c, held):
        for e in range(0, CHUNK, ACCS):
            to = [src_ref[c * CHUNK + e + k] for k in range(ACCS)]
            new = [accs[k][pl.ds(to[k], 1), :] + held[pl.ds(e + k, 1), :] for k in range(ACCS)]
            for k in range(ACCS):
                accs[k][pl.ds(to[k], 1), :] = new[k]

    def backward(p, carry):
        for half, held, ahead in ((0, picked_a, picked_b), (1, picked_b, picked_a)):
            c = 2 * p + half
            scatter(c, held)
            expand(jnp.minimum(c + 1, last_chunk), ahead)()
        return carry

    expand(0, picked_a)()
    lax.fori_loop(0, pairs, backward, 0)

    def total(at, size):
        value = accs[0][pl.ds(at, size), :]
        for acc in accs[1:]:
            value = value + acc[pl.ds(at, size), :]
        return value

    def fold(b, carry):
        at = pl.multiple_of(b * CHUNK, CHUNK)
        own_ref[pl.ds(at, CHUNK), :] += total(at, CHUNK)
        return carry

    lax.fori_loop(0, local_rows // CHUNK, fold, 0)
    group = CHUNK // slots

    wide_rows = 2 * width
    parts[0:wide_rows, :] = wgrad[:, :width]
    parts[wide_rows : 2 * wide_rows, :] = wgrad[:, width:]
    parts[pl.ds(2 * wide_rows, 1), :] = bias_sum[:, :width]
    parts[pl.ds(2 * wide_rows + 1, 1), :] = bias_sum[:, width:]
    parts[2 * wide_rows + 8 : 2 * wide_rows + 8 + hub_total, :] = total(hub_base, hub_total)
    for j in range(ITEMS):
        item = parts[j * peers : (j + 1) * peers, :]
        high = item.astype(BF16).astype(F32)
        table[pl.ds(j, peers, stride=2 * ITEMS), :] = high
        table[pl.ds(j + ITEMS, peers, stride=2 * ITEMS), :] = item - high

    def emit(b, carry):
        at = pl.multiple_of(b * CHUNK, CHUNK)
        halo = total(pl.multiple_of(local_rows + at, CHUNK), CHUNK).reshape(group, slots, width)
        items = table[pl.ds(at, CHUNK), :].reshape(group, 2 * ITEMS, width)
        send_ref[pl.ds(b * group, group), :, :] = jnp.concatenate([halo, items], axis=1).astype(BF16)
        return carry

    lax.fori_loop(0, halo_rows // CHUNK, emit, 0)


def collect_kernel(rows_ref, own_ref, back_ref, sum_ref, rows_in, *accs):
    local_rows, width = own_ref.shape
    peers, _, _ = back_ref.shape
    slots = rows_ref.shape[0] // peers
    accs[0][...] = own_ref[...]
    for acc in accs[1:]:
        acc[...] = jnp.zeros_like(acc)
    rows_in[...] = back_ref[:, 0:slots, :].astype(F32).reshape(peers * slots, width)

    def chunk(c, carry):
        at = c * CHUNK
        for e in range(0, CHUNK, ACCS):
            to = [rows_ref[at + e + k] for k in range(ACCS)]
            new = [
                accs[k][pl.ds(to[k], 1), :] + rows_in[pl.ds(at + e + k, 1), :]
                for k in range(ACCS)
            ]
            for k in range(ACCS):
                accs[k][pl.ds(to[k], 1), :] = new[k]
        return carry

    lax.fori_loop(0, rows_ref.shape[0] // CHUNK, chunk, 0)

    def fold(b, carry):
        at = pl.multiple_of(b * CHUNK, CHUNK)
        value = accs[0][pl.ds(at, CHUNK), :]
        for acc in accs[1:]:
            value = value + acc[pl.ds(at, CHUNK), :]
        sum_ref[pl.ds(at, CHUNK), :] = value
        return carry

    lax.fori_loop(0, local_rows // CHUNK, fold, 0)


def finish_kernel(
    floor_ref, ids_ref, sum_ref, share_ref, grad_ref, self_ref, neigh_ref, bias_ref, total, items,
):
    local_rows, width = sum_ref.shape
    peers = share_ref.shape[0] // ITEMS
    half = self_ref.shape[0]
    total[...] = sum_ref[...]
    items[...] = share_ref[...].astype(F32)
    floor = floor_ref[0]
    first = first_hub(ids_ref, floor)
    for i in range(HUB_MOST):
        held, to = own_hub(ids_ref, first, floor, local_rows, i)
        item = jnp.where(held, 4 * half + 8 + first + i, 0)
        row = items[pl.ds((item % peers) * ITEMS + item // peers, 1), :]
        total[pl.ds(to, 1), :] += jnp.where(held, row, 0.0)
    grad_ref[...] = total[...].astype(BF16)
    for j in range(2):
        item = items[pl.ds(j, peers, stride=ITEMS), :]
        self_ref[:, j * width : (j + 1) * width] = item[:half]
        neigh_ref[:, j * width : (j + 1) * width] = item[half:]
    for j in range(2):
        bias_ref[:, j * width : (j + 1) * width] = items[pl.ds(j * ITEMS + 2, 1), :]


def exchange(array):
    return lax.all_to_all(array, "vert", split_axis=0, concat_axis=0, tiled=True)


def body(
    feats, w_self, w_neigh, bias, cotangent, send_rows, hub_ids, edge_src, edge_dst, edge_count
):
    local_rows, width = feats.shape
    wide = w_self.shape[1]
    peers = lax.axis_size("vert")
    slots = send_rows.shape[2]
    hubs = hub_ids.shape[0]
    edges = edge_src.shape[1]
    halo_rows = peers * slots
    table_rows = -(-(local_rows + halo_rows + hubs) // 16) * 16
    own = lax.axis_index("vert").astype(jnp.int32).reshape(1)
    rows = send_rows.reshape(halo_rows)

    sent = pl.pallas_call(
        pack_kernel,
        out_shape=jax.ShapeDtypeStruct((peers, slots + HUB_MOST, width), BF16),
        in_specs=[SMEM, SMEM, SMEM, VMEM],
        out_specs=VMEM,
        scratch_shapes=[pltpu.VMEM((local_rows, width), F32), pltpu.VMEM((CHUNK, width), F32)],
        name="pack",
    )(own, hub_ids, rows, feats)
    come = exchange(sent)

    starts = edge_dst[:, ::CHUNK]
    output, own_grad, outgoing = pl.pallas_call(
        layer_kernel,
        out_shape=(
            jax.ShapeDtypeStruct((local_rows, wide), BF16),
            jax.ShapeDtypeStruct((local_rows, width), F32),
            jax.ShapeDtypeStruct((peers, slots + 2 * ITEMS, width), BF16),
        ),
        in_specs=[SMEM, SMEM, SMEM, SMEM] + [VMEM] * 7,
        out_specs=(VMEM, VMEM, VMEM),
        scratch_shapes=[
            pltpu.VMEM((table_rows, width), F32),
            pltpu.VMEM((peers * (slots + HUB_MOST), width), F32),
            pltpu.VMEM((CHUNK, width), F32),
            pltpu.VMEM((CHUNK, width), F32),
            pltpu.VMEM((local_rows + 4 * WINDOW, 2 * width), F32),
            pltpu.VMEM((local_rows + WINDOW, width), BF16),
            pltpu.VMEM((2 * width, wide), BF16),
            pltpu.VMEM((2 * width, wide), F32),
            pltpu.VMEM((ITEMS * peers, width), F32),
        ]
        + [pltpu.VMEM((table_rows, width), F32)] * ACCS,
        compiler_params=pltpu.CompilerParams(vmem_limit_bytes=56 * 1024 * 1024),
        name="layer",
    )(
        edge_count, starts, edge_src.reshape(edges), hub_ids, edge_dst, feats, come, cotangent,
        w_self, w_neigh, bias.reshape(1, wide),
    )
    back = exchange(outgoing)
    floors = lax.iota(jnp.int32, 8) + own * local_rows
    summed = jnp.sum(back[:, slots:].astype(F32), axis=0)
    items = (summed[:ITEMS] + summed[ITEMS:]).astype(BF16)[None]
    items = exchange(jnp.broadcast_to(items, (peers, ITEMS, width)))
    sums = pl.pallas_call(
        collect_kernel,
        out_shape=jax.ShapeDtypeStruct((local_rows, width), F32),
        in_specs=[SMEM, VMEM, VMEM],
        out_specs=VMEM,
        scratch_shapes=[pltpu.VMEM((halo_rows, width), F32)]
        + [pltpu.VMEM((local_rows, width), F32)] * ACCS,
        name="collect",
    )(rows, own_grad, back)
    grad_feats, grad_self, grad_neigh, grad_bias = pl.pallas_call(
        finish_kernel,
        out_shape=(
            jax.ShapeDtypeStruct((local_rows, width), BF16),
            jax.ShapeDtypeStruct((width, wide), F32),
            jax.ShapeDtypeStruct((width, wide), F32),
            jax.ShapeDtypeStruct((1, wide), F32),
        ),
        in_specs=[SMEM, SMEM, VMEM, VMEM],
        out_specs=(VMEM,) * 4,
        scratch_shapes=[
            pltpu.VMEM((local_rows, width), F32),
            pltpu.VMEM((peers * ITEMS, width), F32),
        ],
        name="finish",
    )(floors, hub_ids, sums, items.reshape(peers * ITEMS, width))
    return (output, grad_feats, grad_self, grad_neigh, grad_bias.reshape(wide))


def solution(mesh):
    in_specs = (
        P("vert", None),
        P(),
        P(),
        P(),
        P("vert", None),
        P("vert", None, None),
        P(),
        P("vert", None),
        P("vert", None),
        P("vert"),
    )
    out_specs = (P("vert", None), P("vert", None), P(), P(), P())
    return jax.shard_map(body, mesh=mesh, in_specs=in_specs, out_specs=out_specs, check_vma=False)
```
